8 devices in a mesh: dp: 2 (over y, z), tp: 4 (over x, core).
Axes of the slice: x: 2, y: 2, z: 1, core: 2. Of those that a mesh axis runs over, the one named last changes fastest.
Arguments:
- x: bfloat16 [1024, 16384], P(('dp', 'tp')), parts along dimension 0
- gain: bfloat16 [16384], replicated
- wq: bfloat16 [16384, 16384], P(None, 'tp')
- wk: bfloat16 [16384, 16384], P(None, 'tp')
- wv: bfloat16 [16384, 16384], P(None, 'tp')
- wo: bfloat16 [16384, 16384], P('tp')
Outputs:
- output: bfloat16 [1024, 16384], P(('dp', 'tp')), parts along dimension 0
There are 2 independent parts. The reference program is written for one: setup_inputs(seed, part) draws one part's arguments, and reference() takes and returns one part's arrays. A program takes and returns all parts, laid end to end along the dimension named above; an argument that names none is the same for every part.
All inputs are finite; a program needn't handle non-finite values.
Results may differ from the reference program's by a relative error of at most 0.012.
Values are sent between devices in bfloat16 or wider.
A program may use at most 2 GiB of HBM per device.

```python
import jax
import jax.numpy as jnp
from jax import lax

ROWS = 512
D = 16384
HEADS = 128
KV_HEADS = 128
HEAD = 128
THETA = 10000


def setup_inputs(seed: int = 0, part: int = 0) -> dict:
    kx, kn, kq, kk, kv, ko = jax.random.split(jax.random.key(seed), 6)

    def weights(key, rows, columns):
        return jax.random.normal(key, (rows, columns), jnp.float32) * rows**-0.5

    drawn = {
        "x": jax.random.normal(jax.random.fold_in(kx, part), (ROWS, D), jnp.float32),
        "gain": 1 + 0.1 * jax.random.normal(kn, (D,), jnp.float32),
        "wq": 2 * weights(kq, D, HEADS * HEAD),
        "wk": 2 * weights(kk, D, KV_HEADS * HEAD),
        "wv": 4 * weights(kv, D, KV_HEADS * HEAD),
        "wo": weights(ko, HEADS * HEAD, D),
    }
    return {k: v.astype(jnp.bfloat16) for k, v in drawn.items()}


def normed(x, gain):
    wide = x.astype(jnp.float32)
    scale = lax.rsqrt(jnp.mean(wide * wide, -1, keepdims=True) + 1e-6)
    return (wide * scale * gain.astype(jnp.float32)).astype(jnp.bfloat16)


def turned(t, place, theta):
    half = t.shape[-1] // 2
    angle = place.astype(jnp.float32)[:, None] * theta ** (-jnp.arange(half, dtype=jnp.float32) / half)
    cos, sin = jnp.cos(angle)[:, None], jnp.sin(angle)[:, None]
    a, b = t[..., :half].astype(jnp.float32), t[..., half:].astype(jnp.float32)
    return jnp.concatenate([a * cos - b * sin, b * cos + a * sin], -1).astype(jnp.bfloat16)


def matmul(a, w):
    return jnp.dot(a, w, preferred_element_type=jnp.float32).astype(jnp.bfloat16)


def einsum(form, a, b):
    return jnp.einsum(form, a.astype(jnp.float32), b.astype(jnp.float32))


def attention(q, k, v):
    scores = einsum("tgsd,ugd->gstu", q, k) * q.shape[-1] ** -0.5
    token = jnp.arange(q.shape[0])
    scores = jnp.where(token[:, None] >= token, scores, -jnp.inf)
    weights = jax.nn.softmax(scores, -1).astype(jnp.bfloat16)
    return einsum("gstu,ugd->tgsd", weights, v).astype(jnp.bfloat16)


def reference(x, gain, wq, wk, wv, wo):
    a, place = normed(x, gain), jnp.arange(ROWS)
    q = turned(matmul(a, wq).reshape(ROWS, HEADS, HEAD), place, THETA).reshape(ROWS, KV_HEADS, -1, HEAD)
    k = turned(matmul(a, wk).reshape(ROWS, KV_HEADS, HEAD), place, THETA)
    v = matmul(a, wv).reshape(ROWS, KV_HEADS, HEAD)
    seen = attention(q, k, v).reshape(ROWS, HEADS * HEAD)
    return (x.astype(jnp.float32) + jnp.dot(seen, wo, preferred_element_type=jnp.float32)).astype(jnp.bfloat16)
```

```python
import functools

import jax
import jax.numpy as jnp
import numpy as np
from jax import lax
from jax.experimental import pallas as pl
from jax.experimental.pallas import tpu as pltpu
from jax.sharding import PartitionSpec as P

HEAD = 128
THETA = 10000
LOG2E = 1.4426950408889634
HIDDEN = -1e30
MESH = pl.DeviceIdType.MESH
BF16, F32 = jnp.bfloat16, jnp.float32

D = 16384
ROWS = 512
OWN = 128
WIDE = 4096
KC = 1024
NB = 512
CHUNKS = D // KC
BLOCKS = WIDE // NB
OUTS = D // NB
KPARTS = WIDE // KC
LAG = 8
XS, CS, PS = 8, 16, 4


def _dot(a, b, ca=1, cb=0):
    return lax.dot_general(a, b, (((ca,), (cb,)), ((), ())), preferred_element_type=F32)


def _al(i, n):
    return pl.multiple_of(i * n, n)


def kernel(x_ref, gain_ref, cos_ref, sin_ref, wq_ref, wk_ref, wv_ref, wo_ref, o_ref, xa, acc, wb, xres, csend, psend, scale_s,
           x_sem, w_sem, gp_send, gp_recv, gc_send, gc_recv, gf_send, gf_recv, ps_send, ps_recv, cs_send, cs_recv, res_sem, out_sem,
           ready_p, ready_c):
    t = lax.axis_index("tp")
    chip, core = t // 2, t % 2
    partner, peer = chip * 2 + 1 - core, (1 - chip) * 2 + core
    own = pl.ds(_al(t, OWN), OWN)
    theirs = pl.ds(_al(peer, OWN), OWN)

    def load_x(c):
        return pltpu.make_async_copy(x_ref.at[:, pl.ds(_al(c, KC), KC)], xa.at[c, own, :], x_sem.at[c])

    lax.fori_loop(0, CHUNKS, lambda c, _: load_x(c).start(), None)

    def proj_tile(w_ref, c, i, at):
        return pltpu.make_async_copy(w_ref.at[pl.ds(_al(c, KC), KC), pl.ds(i * NB, NB)], wb.at[at + i], w_sem.at[at + i])

    def start_proj(s):
        c, n, at = s // 3, s % 3, (s % 2) * BLOCKS
        for m, w_ref in enumerate((wq_ref, wk_ref, wv_ref)):
            @pl.when(n == m)
            def _():
                for i in range(BLOCKS):
                    proj_tile(w_ref, c, i, at).start()

    def wait_proj(s):
        at = (s % 2) * BLOCKS
        for i in range(BLOCKS):
            proj_tile(wq_ref, 0, i, at).wait()

    def out_tile(j, i):
        at = (j % 4) * KPARTS + i
        return pltpu.make_async_copy(wo_ref.at[pl.ds(i * KC, KC), pl.ds(_al(j, NB), NB)], wb.at[at], w_sem.at[at])

    def start_out(j):
        for i in range(KPARTS):
            out_tile(j, i).start()

    def send(src, dst, send_sem, recv_sem, to):
        return pltpu.make_async_remote_copy(src_ref=src, dst_ref=dst, send_sem=send_sem, recv_sem=recv_sem, device_id={"tp": to},
                                            device_id_type=MESH)

    def to_partner(c):
        return send(xa.at[c, own, :], xa.at[c, own, :], gp_send.at[c], gp_recv.at[c], partner)

    def to_peer(c):
        return send(xa.at[c, own, :], xa.at[c, own, :], gc_send.at[c], gc_recv.at[c], peer)

    def forward(c):
        return send(xa.at[c, theirs, :], xa.at[c, theirs, :], gf_send.at[c], gf_recv.at[c], partner)

    barrier = pltpu.get_barrier_semaphore()
    for to in (partner, peer):
        pl.semaphore_signal(barrier, inc=1, device_id={"tp": to}, device_id_type=MESH)

    start_proj(0)

    def squares(c, total):
        load_x(c).wait()
        v = xa[c, own, :].astype(F32)
        v = v * v
        for i in range(0, KC, 128):
            total = total + v[:, i : i + 128]
        return total

    total = lax.fori_loop(0, CHUNKS, squares, jnp.zeros((OWN, 128), F32))
    scale_s[...] = jnp.broadcast_to(lax.rsqrt(jnp.sum(total, axis=1, keepdims=True) * (1 / D) + 1e-6), (OWN, 128))
    pl.semaphore_wait(barrier, 2)

    def norm(c):
        v = xa[c, own, :].astype(F32)
        scale = jnp.concatenate([scale_s[...]] * (KC // 128), axis=1)
        xa[c, own, :] = (v * scale * gain_ref[c]).astype(BF16)

    def share(c):
        to_peer(c).start()
        to_partner(c).start()

    norm(0)

    def norm_and_share(c, _):
        norm(c)
        share(c - 1)

    lax.fori_loop(1, CHUNKS, norm_and_share, None)

    def clear(i, _):
        acc[i] = jnp.zeros((ROWS, NB), F32)

    lax.fori_loop(0, 3 * BLOCKS, clear, None)
    share(CHUNKS - 1)

    def pass_on(c):
        to_peer(c).wait_recv()
        forward(c).start()

    pass_on(0)

    steps = 3 * CHUNKS

    def project(s, _):
        c, n, at = s // 3, s % 3, (s % 2) * BLOCKS

        @pl.when(s + 1 < steps)
        def _():
            start_proj(s + 1)

        @pl.when(s + 1 == steps)
        def _():
            start_out(0)
            start_out(1)

        @pl.when(n == 0)
        def _():
            to_partner(c).wait_recv()
            forward(c).wait_recv()

        @pl.when((n == 1) & (c + 1 < CHUNKS))
        def _():
            pass_on(c + 1)

        wait_proj(s)
        for i in range(BLOCKS):
            acc[n * BLOCKS + i] += _dot(xa[c], wb[at + i])

    lax.fori_loop(0, steps, project, None)
    start_out(2)
    start_out(3)

    def sent(c, _):
        to_partner(c).wait_send()
        to_peer(c).wait_send()
        forward(c).wait_send()

    lax.fori_loop(0, CHUNKS, sent, None)
    pl.semaphore_signal(ready_p, inc=1, device_id={"tp": partner}, device_id_type=MESH)
    pl.semaphore_signal(ready_c, inc=1, device_id={"tp": peer}, device_id_type=MESH)

    def turned(v):
        v = v.astype(BF16).astype(F32)
        return (v * cos_ref[...] + pltpu.roll(v, HEAD // 2, 1) * sin_ref[...]).astype(BF16)

    half = ROWS // 2
    seen_mask = lax.broadcasted_iota(jnp.int32, (half, half), 0) >= lax.broadcasted_iota(jnp.int32, (half, half), 1)
    e = HEAD**-0.5 * LOG2E

    def attend(b, _):
        for u in range(NB // HEAD):
            lanes = slice(u * HEAD, (u + 1) * HEAD)
            q = turned(acc[b, :, lanes])
            k = turned(acc[BLOCKS + b, :, lanes])
            v = jnp.concatenate([acc[2 * BLOCKS + b, :, lanes].astype(BF16), jnp.ones((ROWS, HEAD), BF16)], axis=1)
            for qb in range(2):
                keys = (qb + 1) * half
                s = _dot(q[qb * half : keys], k[:keys], 1, 1)
                cut = jnp.where(seen_mask, s[:, keys - half :], HIDDEN)
                s = cut if qb == 0 else jnp.concatenate([s[:, :half], cut], axis=1)
                p = jnp.exp2((s - jnp.max(s, axis=1, keepdims=True)) * e).astype(BF16)
                o = _dot(p, v[:keys])
                o = (o[:, :HEAD] * (1 / o[:, HEAD:])).astype(BF16)
                for k_core in range(2):
                    place = jnp.where(core == k_core, 2, 0) + jnp.where(chip == qb, 1, 0)
                    xa[b // 2, pl.ds(_al(place, OWN), OWN), pl.ds(_al((b % 2) * 4 + u, HEAD), HEAD)] = o[k_core * OWN : (k_core + 1) * OWN]

    lax.fori_loop(0, BLOCKS, attend, None)

    def partner_slot(j):
        return xa.at[4 + j // 4, pl.ds(_al(j % 2, 2 * OWN), 2 * OWN), pl.ds(_al((j // 2) % 2, NB), NB)]

    def peer_slot(j):
        return xa.at[12 + j // 8, pl.ds(_al(j % 4, OWN), OWN), pl.ds(_al((j // 4) % 2, NB), NB)]

    def terms(j):
        return send(psend.at[j % PS], partner_slot(j), ps_send.at[j % PS], ps_recv.at[j], partner)

    def sums(j):
        return send(csend.at[j % CS], peer_slot(j), cs_send.at[j % CS], cs_recv.at[j], peer)

    def load_res(j):
        return pltpu.make_async_copy(x_ref.at[:, pl.ds(_al(j, NB), NB)], xres.at[j % XS], res_sem.at[j % XS])

    def put(j):
        return pltpu.make_async_copy(xres.at[j % XS], o_ref.at[:, pl.ds(_al(j, NB), NB)], out_sem.at[j % XS])

    for j in range(XS // 2):
        load_res(j).start()

    def mine(j):
        return acc.at[j // 2, pl.ds(_al(j % 2, 2 * OWN), 2 * OWN), :]

    def combine(j):
        terms(j).wait_recv()

        @pl.when(j >= CS)
        def _():
            sums(j - CS).wait_send()

        kept, got = mine(j), partner_slot(j)
        csend[j % CS] = (kept[:OWN, :] + got[:OWN, :].astype(F32)).astype(BF16)
        kept[OWN:, :] = kept[OWN:, :] + got[OWN:, :].astype(F32)
        sums(j).start()

    def finish(j):
        sums(j).wait_recv()
        load_res(j).wait()
        r = j % XS
        xres[r] = (xres[r].astype(F32) + (mine(j)[OWN:, :] + peer_slot(j)[...].astype(F32))).astype(BF16)
        put(j).start()

        @pl.when(j + XS // 2 < OUTS)
        def _():
            @pl.when(j >= XS // 2)
            def _():
                put(j - XS // 2).wait()

            load_res(j + XS // 2).start()

    pl.semaphore_wait(ready_p, 1)
    pl.semaphore_wait(ready_c, 1)

    def project_out(j, _):
        @pl.when((j >= 1) & (j + 3 < OUTS))
        def _():
            start_out(j + 3)

        for i in range(KPARTS):
            out_tile(j, i).wait()

        @pl.when(j >= PS)
        def _():
            terms(j - PS).wait_send()

        at = (j % 4) * KPARTS
        y = _dot(xa[0], wb[at])
        for i in range(1, KPARTS):
            y = y + _dot(xa[i], wb[at + i])
        psend[j % PS] = y[: 2 * OWN].astype(BF16)
        mine(j)[...] = y[2 * OWN :]
        terms(j).start()

        @pl.when(j >= 1)
        def _():
            combine(j - 1)

        @pl.when(j >= 1 + LAG)
        def _():
            finish(j - 1 - LAG)

    lax.fori_loop(0, OUTS, project_out, None)
    combine(OUTS - 1)
    lax.fori_loop(OUTS - 1 - LAG, OUTS, lambda j, _: finish(j), None)

    for j in range(OUTS - XS, OUTS):
        put(j).wait()
    lax.fori_loop(OUTS - PS, OUTS, lambda j, _: terms(j).wait_send(), None)
    lax.fori_loop(OUTS - CS, OUTS, lambda j, _: sums(j).wait_send(), None)


def tables():
    half = HEAD // 2
    angle = np.arange(ROWS, dtype=np.float32)[:, None] * (THETA ** (-np.arange(half, dtype=np.float32) / half)).astype(np.float32)
    cos, sin = np.cos(angle.astype(np.float64)), np.sin(angle.astype(np.float64))
    return np.concatenate([cos, cos], 1).astype(np.float32), np.concatenate([-sin, sin], 1).astype(np.float32)


def solution(mesh):
    def step(x, gain, wq, wk, wv, wo):
        cos, sin = tables()
        whole = pl.BlockSpec(memory_space=pltpu.VMEM)
        away = pl.BlockSpec(memory_space=pl.ANY)
        dma = pltpu.SemaphoreType.DMA
        return pl.pallas_call(
            kernel,
            out_shape=jax.ShapeDtypeStruct((OWN, D), BF16),
            in_specs=[away, whole, whole, whole, away, away, away, away],
            out_specs=away,
            scratch_shapes=[
                pltpu.VMEM((CHUNKS, ROWS, KC), BF16),
                pltpu.VMEM((3 * BLOCKS, ROWS, NB), F32),
                pltpu.VMEM((16, KC, NB), BF16),
                pltpu.VMEM((XS, OWN, NB), BF16),
                pltpu.VMEM((CS, OWN, NB), BF16),
                pltpu.VMEM((PS, 2 * OWN, NB), BF16),
                pltpu.VMEM((OWN, 128), F32),
                dma((CHUNKS,)),
                dma((16,)),
                dma((CHUNKS,)), dma((CHUNKS,)), dma((CHUNKS,)), dma((CHUNKS,)), dma((CHUNKS,)), dma((CHUNKS,)),
                dma((PS,)), dma((OUTS,)), dma((CS,)), dma((OUTS,)),
                dma((XS,)), dma((XS,)),
                pltpu.SemaphoreType.REGULAR,
                pltpu.SemaphoreType.REGULAR,
            ],
            compiler_params=pltpu.CompilerParams(collective_id=0, has_side_effects=True, vmem_limit_bytes=67_000_000),
            cost_estimate=pl.CostEstimate(flops=8 * ROWS * D * WIDE, bytes_accessed=8 * D * WIDE, transcendentals=0),
        )(x, gain.astype(F32).reshape(CHUNKS, 1, KC), jnp.asarray(cos), jnp.asarray(sin), wq, wk, wv, wo)

    tokens, columns = P(("dp", "tp"), None), P(None, "tp")
    return jax.shard_map(
        step,
        mesh=mesh,
        in_specs=(tokens, P(None), columns, columns, columns, P("tp", None)),
        out_specs=tokens,
        check_vma=False,
    )
```

```python
import functools

import jax
import jax.numpy as jnp
import numpy as np
from jax import lax
from jax.experimental import pallas as pl
from jax.experimental.pallas import tpu as pltpu
from jax.sharding import PartitionSpec as P

HEAD = 128
THETA = 10000
LOG2E = 1.4426950408889634
HIDDEN = -1e30
MESH = pl.DeviceIdType.MESH
BF16, F32 = jnp.bfloat16, jnp.float32

D = 16384
ROWS = 512
OWN = 128
WIDE = 4096
KC = 1024
NB = 512
CHUNKS = D // KC
BLOCKS = WIDE // NB
OUTS = D // NB
KPARTS = WIDE // KC
LAG = 12
CS, PS = 8, 2
UNITS = 12
EARLY = 8


def _dot(a, b, ca=1, cb=0):
    return lax.dot_general(a, b, (((ca,), (cb,)), ((), ())), preferred_element_type=F32)


def _al(i, n):
    return pl.multiple_of(i * n, n)


def kernel(x_ref, gain_ref, cos_ref, sin_ref, wq_ref, wk_ref, wv_ref, wo_ref, o_ref, xa, acc, wb, csend, psend, scale_s,
           x_sem, w_sem, gp_send, gp_recv, gc_send, gc_recv, gf_send, gf_recv, ps_send, ps_recv, cs_send, cs_recv,
           ready_p, ready_c):
    t = lax.axis_index("tp")
    chip, core = t // 2, t % 2
    partner, peer = chip * 2 + 1 - core, (1 - chip) * 2 + core
    own = pl.ds(_al(t, OWN), OWN)
    theirs = pl.ds(_al(peer, OWN), OWN)

    def load_x(c):
        return pltpu.make_async_copy(x_ref.at[:, pl.ds(_al(c, KC), KC)], o_ref.at[:, pl.ds(_al(c, KC), KC)], x_sem.at[c])

    lax.fori_loop(0, CHUNKS, lambda c, _: load_x(c).start(), None)

    def proj_tile(w_ref, c, at, i, column):
        return pltpu.make_async_copy(w_ref.at[pl.ds(_al(c, KC), KC), pl.ds(column, NB)], wb.at[at + i], w_sem.at[at + i])

    def start_unit(u):
        n, at = (u // 2) % 3, (u % 4) * KPARTS
        for m, w_ref in enumerate((wq_ref, wk_ref, wv_ref)):
            @pl.when(n == m)
            def _():
                for i in range(KPARTS):
                    proj_tile(w_ref, u // UNITS, at, i, pl.multiple_of((u % 2) * (WIDE // 2) + i * NB, NB)).start()

    def start_proj(s):
        c, n, at = (s - 3) // 3, s % 3, (s % 2) * BLOCKS
        for m, w_ref in enumerate((wq_ref, wk_ref, wv_ref)):
            @pl.when(n == m)
            def _():
                for i in range(BLOCKS):
                    proj_tile(w_ref, c, at, i, i * NB).start()

    def wait_tiles(at, count):
        for i in range(count):
            proj_tile(wq_ref, 0, at, i, 0).wait()

    def out_tile(j, i):
        at = ((j + 2) % 4) * KPARTS + i
        return pltpu.make_async_copy(wo_ref.at[pl.ds(i * KC, KC), pl.ds(_al(j % OUTS, NB), NB)], wb.at[at], w_sem.at[at])

    def start_out(j):
        for i in range(KPARTS):
            out_tile(j, i).start()

    def send(src, dst, send_sem, recv_sem, to):
        return pltpu.make_async_remote_copy(src_ref=src, dst_ref=dst, send_sem=send_sem, recv_sem=recv_sem, device_id={"tp": to},
                                            device_id_type=MESH)

    def to_partner(c):
        return send(xa.at[c, own, :], xa.at[c, own, :], gp_send.at[c], gp_recv.at[c], partner)

    def to_peer(c):
        return send(xa.at[c, own, :], xa.at[c, own, :], gc_send.at[c], gc_recv.at[c], peer)

    def forward(c):
        return send(xa.at[c, theirs, :], xa.at[c, theirs, :], gf_send.at[c], gf_recv.at[c], partner)

    barrier = pltpu.get_barrier_semaphore()
    for to in (partner, peer):
        pl.semaphore_signal(barrier, inc=1, device_id={"tp": to}, device_id_type=MESH)

    def squares(c, total):
        load_x(c).wait()
        v = o_ref[:, pl.ds(_al(c, KC), KC)].astype(F32)
        v = v * v
        for i in range(0, KC, 128):
            total = total + v[:, i : i + 128]
        return total

    total = lax.fori_loop(0, CHUNKS, squares, jnp.zeros((OWN, 128), F32))
    for u in range(3):
        start_unit(u)
    scale_s[...] = jnp.broadcast_to(lax.rsqrt(jnp.sum(total, axis=1, keepdims=True) * (1 / D) + 1e-6), (OWN, 128))
    pl.semaphore_wait(barrier, 2)

    def norm(c):
        v = o_ref[:, pl.ds(_al(c, KC), KC)].astype(F32)
        scale = jnp.concatenate([scale_s[...]] * (KC // 128), axis=1)
        xa[c, own, :] = (v * scale * gain_ref[pl.ds(_al(c, KC), KC)].astype(F32).reshape(1, KC)).astype(BF16)

    def share(c):
        to_peer(c).start()
        to_partner(c).start()

    norm(0)
    norm(1)
    share(0)

    def norm_rest(c, _):
        norm(c)

        @pl.when(c == 2)
        def _():
            share(1)

    lax.fori_loop(2, CHUNKS, norm_rest, None)

    def pass_on(c):
        to_peer(c).wait_recv()
        forward(c).start()

    last = 3 * CHUNKS + 2

    def project_first(u, _):
        at = (u % 4) * KPARTS

        @pl.when(u + 3 < UNITS + 2)
        def _():
            start_unit(u + 3)

        @pl.when(u % 4 == 3)
        def _():
            share(u // 4 + 2)

        @pl.when(u == 0)
        def _():
            to_partner(0).wait_recv()

        @pl.when(u == 5)
        def _():
            pass_on(0)

        @pl.when(u == 6)
        def _():
            forward(0).wait_recv()

        @pl.when(u == 9)
        def _():
            pass_on(1)

        wait_tiles(at, KPARTS)
        rows = pl.ds(_al(jnp.where(u < 6, chip, 1 - chip), 2 * OWN), 2 * OWN)
        for i in range(KPARTS):
            acc[(u % 6) * KPARTS + i, rows, :] = _dot(xa[0, rows, :], wb[at + i])

    lax.fori_loop(0, UNITS, project_first, None)

    def project(s, _):
        c, n, at = (s - 3) // 3, s % 3, (s % 2) * BLOCKS

        @pl.when(s < last)
        def _():
            start_proj(s + 1)

        @pl.when(s == last)
        def _():
            start_out(0)
            start_out(1)

        @pl.when(s - 1 < CHUNKS)
        def _():
            share(s - 1)

        @pl.when(n == 0)
        def _():
            to_partner(c).wait_recv()
            forward(c).wait_recv()

        @pl.when((n == 1) & (c + 1 < CHUNKS))
        def _():
            pass_on(c + 1)

        wait_tiles(at, BLOCKS)
        for i in range(BLOCKS):
            acc[n * BLOCKS + i] += _dot(xa[c], wb[at + i])

    lax.fori_loop(UNITS // 2, last + 1, project, None)
    start_out(2)
    start_out(3)

    def sent(c, _):
        to_partner(c).wait_send()
        to_peer(c).wait_send()
        forward(c).wait_send()

    lax.fori_loop(0, CHUNKS, sent, None)
    pl.semaphore_signal(ready_p, inc=1, device_id={"tp": partner}, device_id_type=MESH)
    pl.semaphore_signal(ready_c, inc=1, device_id={"tp": peer}, device_id_type=MESH)

    def turned(v):
        v = v.astype(BF16).astype(F32)
        return lambda cos, sin: (v * cos + pltpu.roll(v, HEAD // 2, 1) * sin).astype(BF16)

    half = ROWS // 2
    seen_mask = lax.broadcasted_iota(jnp.int32, (half, half), 0) >= lax.broadcasted_iota(jnp.int32, (half, half), 1)
    e = HEAD**-0.5 * LOG2E

    def attend(qb):
        keys, first = (qb + 1) * half, qb * half

        def heads(b, _):
            def scores(u):
                lanes = slice(u * HEAD, (u + 1) * HEAD)
                q = turned(acc[b, first:keys, lanes])(cos_ref[first:keys, :], sin_ref[first:keys, :])
                k = turned(acc[BLOCKS + b, :keys, lanes])(cos_ref[:keys, :], sin_ref[:keys, :])
                return _dot(q, k, 1, 1)

            def result(u, s):
                lanes = slice(u * HEAD, (u + 1) * HEAD)
                v = jnp.concatenate([acc[2 * BLOCKS + b, :keys, lanes].astype(BF16), jnp.ones((keys, HEAD), BF16)], axis=1)
                cut = jnp.where(seen_mask, s[:, first:], HIDDEN)
                s = cut if qb == 0 else jnp.concatenate([s[:, :first], cut], axis=1)
                p = jnp.exp2((s - jnp.max(s, axis=1, keepdims=True)) * e).astype(BF16)
                o = _dot(p, v)
                o = (o[:, :HEAD] * (1 / o[:, HEAD:])).astype(BF16)
                for k_core in range(2):
                    place = jnp.where(chip == qb, 2, 0) + jnp.where(core == k_core, 1, 0)
                    xa[b // 2, pl.ds(_al(place, OWN), OWN), pl.ds(_al((b % 2) * 4 + u, HEAD), HEAD)] = o[k_core * OWN : (k_core + 1) * OWN]

            s = scores(0)
            for u in range(NB // HEAD):
                after = scores(u + 1) if u + 1 < NB // HEAD else None
                result(u, s)
                s = after

        lax.fori_loop(0, BLOCKS, heads, None)

    def attend_for(whose):
        for qb in range(2):
            @pl.when(whose == qb)
            def _():
                attend(qb)

    attend_for(1 - chip)

    def piece(part, j):
        return xa.at[part + j // 8, pl.ds(_al(j % 4, OWN), OWN), pl.ds(_al((j // 4) % 2, NB), NB)]

    def terms(h, j):
        return send(psend.at[h, j % PS], piece(4 + 4 * h, j), ps_send.at[h, j % PS], ps_recv.at[h, j], partner)

    def sums(j):
        return send(csend.at[j % CS], piece(12, j), cs_send.at[j % CS], cs_recv.at[j], peer)

    def mine(h, j):
        return acc.at[j // 2, pl.ds(_al((chip + 1 + h) % 2 * 2 + j % 2, OWN), OWN), :]

    def keep(h, j, y):
        psend[h, j % PS] = y[:OWN].astype(BF16)
        mine(h, j)[...] = y[OWN:]

    def combine(j):
        terms(0, j).wait_recv()

        @pl.when(j >= CS)
        def _():
            sums(j - CS).wait_send()

        csend[j % CS] = (mine(0, j)[...] + piece(4, j)[...].astype(F32)).astype(BF16)
        sums(j).start()

    def finish(j):
        terms(1, j).wait_recv()
        sums(j).wait_recv()
        columns = pl.ds(_al(j, NB), NB)
        total = mine(1, j)[...] + piece(8, j)[...].astype(F32) + piece(12, j)[...].astype(F32)
        o_ref[:, columns] = (o_ref[:, columns].astype(F32) + total).astype(BF16)

    def product(q, rows):
        at = ((q + 2) % 4) * KPARTS
        y = _dot(xa[0, rows, :], wb[at])
        for i in range(1, KPARTS):
            y = y + _dot(xa[i, rows, :], wb[at + i])
        return y

    def tiles(q):
        @pl.when((q >= 1) & (q + 3 < OUTS + EARLY))
        def _():
            start_out(q + 3)

        for i in range(KPARTS):
            out_tile(q, i).wait()

    pl.semaphore_wait(ready_p, 1)
    pl.semaphore_wait(ready_c, 1)

    def other_rows(j, _):
        tiles(j)

        @pl.when(j >= PS)
        def _():
            terms(0, j - PS).wait_send()

        keep(0, j, product(j, slice(0, half)))
        terms(0, j).start()

        @pl.when(j >= 1)
        def _():
            combine(j - 1)

    def all_rows(j, _):
        tiles(j)
        terms(0, j - PS).wait_send()

        @pl.when(j - PS >= EARLY)
        def _():
            terms(1, j - PS).wait_send()

        y = product(j, slice(0, ROWS))
        keep(0, j, y[:half])
        keep(1, j, y[half:])
        terms(0, j).start()
        terms(1, j).start()
        combine(j - 1)

        @pl.when(j - 1 - LAG >= EARLY)
        def _():
            finish(j - 1 - LAG)

    def own_rows(j, _):
        tiles(j + OUTS)

        @pl.when(j < PS)
        def _():
            terms(1, j + OUTS - PS).wait_send()

        @pl.when(j >= PS)
        def _():
            terms(1, j - PS).wait_send()

        keep(1, j, product(j + OUTS, slice(half, ROWS)))
        terms(1, j).start()
        finish(j + OUTS - 1 - LAG)

    lax.fori_loop(0, EARLY, other_rows, None)
    attend_for(chip)
    lax.fori_loop(EARLY, OUTS, all_rows, None)
    combine(OUTS - 1)
    lax.fori_loop(0, EARLY, own_rows, None)
    lax.fori_loop(0, EARLY, lambda j, _: finish(j), None)
    lax.fori_loop(OUTS + EARLY - 1 - LAG, OUTS, lambda j, _: finish(j), None)
    lax.fori_loop(OUTS - PS, OUTS, lambda j, _: terms(0, j).wait_send(), None)
    lax.fori_loop(EARLY - PS, EARLY, lambda j, _: terms(1, j).wait_send(), None)
    lax.fori_loop(OUTS - CS, OUTS, lambda j, _: sums(j).wait_send(), None)


def tables():
    half = HEAD // 2
    angle = np.arange(ROWS, dtype=np.float32)[:, None] * (THETA ** (-np.arange(half, dtype=np.float32) / half)).astype(np.float32)
    cos, sin = np.cos(angle.astype(np.float64)), np.sin(angle.astype(np.float64))
    return np.concatenate([cos, cos], 1).astype(np.float32), np.concatenate([-sin, sin], 1).astype(np.float32)


def solution(mesh):
    def step(x, gain, wq, wk, wv, wo):
        cos, sin = tables()
        whole = pl.BlockSpec(memory_space=pltpu.VMEM)
        away = pl.BlockSpec(memory_space=pl.ANY)
        dma = pltpu.SemaphoreType.DMA
        return pl.pallas_call(
            kernel,
            out_shape=pltpu.VMEM((OWN, D), BF16),
            in_specs=[away, whole, whole, whole, away, away, away, away],
            out_specs=whole,
            scratch_shapes=[
                pltpu.VMEM((CHUNKS, ROWS, KC), BF16),
                pltpu.VMEM((3 * BLOCKS, ROWS, NB), F32),
                pltpu.VMEM((16, KC, NB), BF16),
                pltpu.VMEM((CS, OWN, NB), BF16),
                pltpu.VMEM((2, PS, OWN, NB), BF16),
                pltpu.VMEM((OWN, 128), F32),
                dma((CHUNKS,)),
                dma((16,)),
                dma((CHUNKS,)), dma((CHUNKS,)), dma((CHUNKS,)), dma((CHUNKS,)), dma((CHUNKS,)), dma((CHUNKS,)),
                dma((2, PS)), dma((2, OUTS)), dma((CS,)), dma((OUTS,)),
                pltpu.SemaphoreType.REGULAR,
                pltpu.SemaphoreType.REGULAR,
            ],
            compiler_params=pltpu.CompilerParams(collective_id=0, has_side_effects=True, vmem_limit_bytes=62_800_000),
            cost_estimate=pl.CostEstimate(flops=8 * ROWS * D * WIDE, bytes_accessed=8 * D * WIDE, transcendentals=0),
        )(x, gain, jnp.asarray(cos), jnp.asarray(sin), wq, wk, wv, wo)

    tokens, columns = P(("dp", "tp"), None), P(None, "tp")
    return jax.shard_map(
        step,
        mesh=mesh,
        in_specs=(tokens, P(None), columns, columns, columns, P("tp", None)),
        out_specs=tokens,
        check_vma=False,
    )
```

```python
import functools

import jax
import jax.numpy as jnp
import numpy as np
from jax import lax
from jax.experimental import pallas as pl
from jax.experimental.pallas import tpu as pltpu
from jax.sharding import PartitionSpec as P

HEAD = 128
THETA = 10000
LOG2E = 1.4426950408889634
HIDDEN = -1e30
MESH = pl.DeviceIdType.MESH
BF16, F32 = jnp.bfloat16, jnp.float32

D = 16384
ROWS = 512
OWN = 128
WIDE = 4096
KC = 1024
NB = 512
CHUNKS = D // KC
BLOCKS = WIDE // NB
OUTS = D // NB
KPARTS = WIDE // KC
LAG = 12
PS = 2
UNITS = 12
EARLY = 8


def _dot(a, b, ca=1, cb=0):
    return lax.dot_general(a, b, (((ca,), (cb,)), ((), ())), preferred_element_type=F32)


def _al(i, n):
    return pl.multiple_of(i * n, n)


def kernel(x_ref, gain_in, cos_in, sin_in, wq_ref, wk_ref, wv_ref, wo_ref, o_ref, xa, acc, wb, psend, gain_ref, cos_ref,
           sin_ref, x_sem, small_sem, w_sem, gp_send, gp_recv, gc_send, gc_recv, gf_send, gf_recv, ps_send, ps_recv, cs_send, cs_recv,
           ready_p, ready_c):
    t = lax.axis_index("tp")
    chip, core = t // 2, t % 2
    partner, peer = chip * 2 + 1 - core, (1 - chip) * 2 + core
    own = pl.ds(_al(t, OWN), OWN)
    theirs = pl.ds(_al(peer, OWN), OWN)

    def load_x(c):
        return pltpu.make_async_copy(x_ref.at[:, pl.ds(_al(c, KC), KC)], o_ref.at[:, pl.ds(_al(c, KC), KC)], x_sem.at[c])

    small = [pltpu.make_async_copy(a, b, small_sem.at[i]) for i, (a, b) in
             enumerate(((gain_in, gain_ref), (cos_in, cos_ref), (sin_in, sin_ref)))]
    small[0].start()
    lax.fori_loop(0, CHUNKS, lambda c, _: load_x(c).start(), None)

    def slot(i):
        return wb.at[i // 2, :, pl.ds(_al(i % 2, WIDE // 2), WIDE // 2)]

    def start_unit(c, n, u):
        for m, w_ref in enumerate((wq_ref, wk_ref, wv_ref)):
            @pl.when(n == m)
            def _():
                rows, columns = pl.ds(_al(c, KC), KC), pl.ds(_al(u % 2, WIDE // 2), WIDE // 2)
                pltpu.make_async_copy(w_ref.at[rows, columns], slot(u % 4), w_sem.at[u % 4, 0]).start()

    def start_proj(s):
        c, n = (s - 3) // 3, s % 3
        for m, w_ref in enumerate((wq_ref, wk_ref, wv_ref)):
            @pl.when(n == m)
            def _():
                for i in range(2):
                    rows, columns = pl.ds(_al(c, KC), KC), pl.ds(i * (WIDE // 2), WIDE // 2)
                    pltpu.make_async_copy(w_ref.at[rows, columns], slot(s % 2 * 2 + i), w_sem.at[s % 2 * 2 + i, 0]).start()

    def wait_unit(i):
        pltpu.make_async_copy(wq_ref.at[pl.ds(0, KC), pl.ds(0, WIDE // 2)], slot(i), w_sem.at[i, 0]).wait()

    def out_part(j, i):
        at = (j + 2) % 4
        return at // 2, slice(None), pl.ds(_al(at % 2 * KPARTS + i, NB), NB)

    def out_tile(j, i):
        return pltpu.make_async_copy(wo_ref.at[pl.ds(i * KC, KC), pl.ds(_al(j % OUTS, NB), NB)], wb.at[out_part(j, i)], w_sem.at[(j + 2) % 4, i])

    def start_out(j):
        for i in range(KPARTS):
            out_tile(j, i).start()

    def send(src, dst, send_sem, recv_sem, to):
        return pltpu.make_async_remote_copy(src_ref=src, dst_ref=dst, send_sem=send_sem, recv_sem=recv_sem, device_id={"tp": to},
                                            device_id_type=MESH)

    def to_partner(c):
        return send(xa.at[c, own, :], xa.at[c, own, :], gp_send.at[c], gp_recv.at[c], partner)

    def to_peer(c):
        return send(xa.at[c, own, :], xa.at[c, own, :], gc_send.at[c], gc_recv.at[c], peer)

    def forward(c):
        return send(xa.at[c, theirs, :], xa.at[c, theirs, :], gf_send.at[c], gf_recv.at[c], partner)

    barrier = pltpu.get_barrier_semaphore()
    for to in (partner, peer):
        pl.semaphore_signal(barrier, inc=1, device_id={"tp": to}, device_id_type=MESH)

    for u in range(3):
        start_unit(0, u // 2, u)

    def squares(c, total):
        load_x(c).wait()
        v = o_ref[:, pl.ds(_al(c, KC), KC)].astype(F32)
        v = v * v
        for i in range(0, KC, 128):
            total = total + v[:, i : i + 128]
        return total

    total = lax.fori_loop(0, CHUNKS, squares, jnp.zeros((OWN, 128), F32))
    scale_ref = acc.at[3 * BLOCKS - 1, pl.ds(0, OWN), pl.ds(0, 128)]
    scale_ref[...] = jnp.broadcast_to(lax.rsqrt(jnp.sum(total, axis=1, keepdims=True) * (1 / D) + 1e-6), (OWN, 128))
    pl.semaphore_wait(barrier, 2)

    def norm(c):
        v = o_ref[:, pl.ds(_al(c, KC), KC)].astype(F32)
        scale = jnp.concatenate([scale_ref[...]] * (KC // 128), axis=1)
        xa[c, own, :] = (v * scale * gain_ref[pl.ds(_al(c, KC), KC)].astype(F32).reshape(1, KC)).astype(BF16)

    def share(c):
        to_peer(c).start()
        to_partner(c).start()

    small[0].wait()
    norm(0)
    norm(1)
    share(0)
    small[1].start()
    small[2].start()

    lax.fori_loop(2, CHUNKS, lambda c, _: norm(c), None)

    def pass_on(c):
        to_peer(c).wait_recv()
        forward(c).start()

    last = 3 * CHUNKS + 2

    def project_first(u, _):
        @pl.when(u + 3 < UNITS + 2)
        def _():
            start_unit((u + 3) // UNITS, (u + 3) // 2 % 3, u + 3)

        @pl.when((u % 3 == 0) & (u > 0))
        def _():
            share(u // 3)

        @pl.when(u == UNITS - 1)
        def _():
            share(4)

        @pl.when(u == 0)
        def _():
            to_partner(0).wait_recv()

        @pl.when(u == 5)
        def _():
            pass_on(0)

        @pl.when(u == 6)
        def _():
            forward(0).wait_recv()

        @pl.when(u == 9)
        def _():
            pass_on(1)

        wait_unit(u % 4)
        rows = pl.ds(_al(jnp.where(u < 6, chip, 1 - chip), 2 * OWN), 2 * OWN)
        for i in range(KPARTS):
            acc[(u % 6) * KPARTS + i, rows, :] = _dot(xa[0, rows, :], wb[u % 4 // 2, :, pl.ds(_al(u % 2 * KPARTS + i, NB), NB)])

    lax.fori_loop(0, UNITS, project_first, None)

    def project(s, _):
        c, n = (s - 3) // 3, s % 3

        @pl.when(s < last)
        def _():
            start_proj(s + 1)

        @pl.when(s == last)
        def _():
            start_out(0)
            start_out(1)

        @pl.when(s - 1 < CHUNKS)
        def _():
            share(s - 1)

        @pl.when(n == 0)
        def _():
            to_partner(c).wait_recv()
            forward(c).wait_recv()

        @pl.when((n == 1) & (c + 1 < CHUNKS))
        def _():
            pass_on(c + 1)

        for i in range(2):
            wait_unit(s % 2 * 2 + i)
        for i in range(BLOCKS):
            acc[n * BLOCKS + i] += _dot(xa[c], wb[s % 2, :, i * NB : (i + 1) * NB])

    lax.fori_loop(UNITS // 2, last + 1, project, None)
    start_out(2)
    start_out(3)

    def sent(c, _):
        to_partner(c).wait_send()
        to_peer(c).wait_send()
        forward(c).wait_send()

    lax.fori_loop(0, CHUNKS, sent, None)
    pl.semaphore_signal(ready_p, inc=1, device_id={"tp": partner}, device_id_type=MESH)
    pl.semaphore_signal(ready_c, inc=1, device_id={"tp": peer}, device_id_type=MESH)

    def turned(v):
        v = v.astype(BF16).astype(F32)
        return lambda cos, sin: (v * cos + pltpu.roll(v, HEAD // 2, 1) * sin).astype(BF16)

    half = ROWS // 2
    seen_mask = lax.broadcasted_iota(jnp.int32, (half, half), 0) >= lax.broadcasted_iota(jnp.int32, (half, half), 1)
    e = HEAD**-0.5 * LOG2E

    def attend(qb):
        keys, first = (qb + 1) * half, qb * half

        def heads(b, _):
            def scores(u):
                lanes = slice(u * HEAD, (u + 1) * HEAD)
                q = turned(acc[b, first:keys, lanes])(cos_ref[first:keys, :], sin_ref[first:keys, :])
                k = turned(acc[BLOCKS + b, :keys, lanes])(cos_ref[:keys, :], sin_ref[:keys, :])
                return _dot(q, k, 1, 1)

            def weights(s):
                cut = jnp.where(seen_mask, s[:, first:], HIDDEN)
                s = cut if qb == 0 else jnp.concatenate([s[:, :first], cut], axis=1)
                return jnp.exp2((s - jnp.max(s, axis=1, keepdims=True)) * e).astype(BF16)

            def result(u, p):
                lanes = slice(u * HEAD, (u + 1) * HEAD)
                v = jnp.concatenate([acc[2 * BLOCKS + b, :keys, lanes].astype(BF16), jnp.ones((keys, HEAD), BF16)], axis=1)
                o = _dot(p, v)
                o = (o[:, :HEAD] * (1 / o[:, HEAD:])).astype(BF16)
                for k_core in range(2):
                    place = jnp.where(chip == qb, 2, 0) + jnp.where(core == k_core, 1, 0)
                    xa[b // 2, pl.ds(_al(place, OWN), OWN), pl.ds(_al((b % 2) * 4 + u, HEAD), HEAD)] = o[k_core * OWN : (k_core + 1) * OWN]

            every = [scores(u) for u in range(NB // HEAD)]
            every = [weights(s) for s in every]
            for u, p in enumerate(every):
                result(u, p)

        lax.fori_loop(0, BLOCKS, heads, None, unroll=2)

    def attend_for(whose):
        for qb in range(2):
            @pl.when(whose == qb)
            def _():
                attend(qb)

    small[1].wait()
    small[2].wait()
    attend_for(1 - chip)

    def piece(part, j):
        return xa.at[part + j // 8, pl.ds(_al(j % 4, OWN), OWN), pl.ds(_al((j // 4) % 2, NB), NB)]

    def terms(h, j):
        return send(psend.at[h, j % PS], piece(4 + 4 * h, j), ps_send.at[h, j % PS], ps_recv.at[h, j], partner)

    def sums(j):
        return send(piece(4, j), piece(12, j), cs_send.at[j], cs_recv.at[j], peer)

    def mine(h, j):
        return acc.at[j // 2, pl.ds(_al((chip + 1 + h) % 2 * 2 + j % 2, OWN), OWN), :]

    def keep(h, j, y):
        psend[h, j % PS] = y[:OWN].astype(BF16)
        mine(h, j)[...] = y[OWN:]

    def combine(j):
        terms(0, j).wait_recv()
        got = piece(4, j)
        got[...] = (mine(0, j)[...] + got[...].astype(F32)).astype(BF16)
        sums(j).start()

    def finish(j):
        terms(1, j).wait_recv()
        sums(j).wait_recv()
        columns = pl.ds(_al(j, NB), NB)
        total = mine(1, j)[...] + piece(8, j)[...].astype(F32) + piece(12, j)[...].astype(F32)
        o_ref[:, columns] = (o_ref[:, columns].astype(F32) + total).astype(BF16)

    def product(q, rows):
        y = _dot(xa[0, rows, :], wb[out_part(q, 0)])
        for i in range(1, KPARTS):
            y = y + _dot(xa[i, rows, :], wb[out_part(q, i)])
        return y

    def tiles(q):
        @pl.when((q >= 1) & (q + 3 < OUTS + EARLY))
        def _():
            start_out(q + 3)

        for i in range(KPARTS):
            out_tile(q, i).wait()

    pl.semaphore_wait(ready_p, 1)
    pl.semaphore_wait(ready_c, 1)

    def other_rows(j, _):
        tiles(j)

        @pl.when(j >= PS)
        def _():
            terms(0, j - PS).wait_send()

        keep(0, j, product(j, slice(0, half)))
        terms(0, j).start()

        @pl.when(j >= 1)
        def _():
            combine(j - 1)

    def all_rows(j, _):
        tiles(j)
        terms(0, j - PS).wait_send()

        @pl.when(j - PS >= EARLY)
        def _():
            terms(1, j - PS).wait_send()

        y = product(j, slice(0, ROWS))
        keep(0, j, y[:half])
        keep(1, j, y[half:])
        terms(0, j).start()
        terms(1, j).start()
        combine(j - 1)

        @pl.when(j - 1 - LAG >= EARLY)
        def _():
            finish(j - 1 - LAG)

    def own_rows(j, _):
        tiles(j + OUTS)

        @pl.when(j < PS)
        def _():
            terms(1, j + OUTS - PS).wait_send()

        @pl.when(j >= PS)
        def _():
            terms(1, j - PS).wait_send()

        keep(1, j, product(j + OUTS, slice(half, ROWS)))
        terms(1, j).start()
        finish(j + OUTS - 1 - LAG)

    lax.fori_loop(0, EARLY, other_rows, None)
    attend_for(chip)
    lax.fori_loop(EARLY, OUTS, all_rows, None)
    combine(OUTS - 1)
    lax.fori_loop(0, EARLY, own_rows, None)
    lax.fori_loop(0, EARLY, lambda j, _: finish(j), None)
    lax.fori_loop(OUTS + EARLY - 1 - LAG, OUTS, lambda j, _: finish(j), None)
    lax.fori_loop(OUTS - PS, OUTS, lambda j, _: terms(0, j).wait_send(), None)
    lax.fori_loop(EARLY - PS, EARLY, lambda j, _: terms(1, j).wait_send(), None)
    lax.fori_loop(0, OUTS, lambda j, _: sums(j).wait_send(), None)


def tables():
    half = HEAD // 2
    angle = np.arange(ROWS, dtype=np.float32)[:, None] * (THETA ** (-np.arange(half, dtype=np.float32) / half)).astype(np.float32)
    cos, sin = np.cos(angle.astype(np.float64)), np.sin(angle.astype(np.float64))
    return np.concatenate([cos, cos], 1).astype(np.float32), np.concatenate([-sin, sin], 1).astype(np.float32)


def solution(mesh):
    def step(x, gain, wq, wk, wv, wo):
        cos, sin = tables()
        whole = pl.BlockSpec(memory_space=pltpu.VMEM)
        away = pl.BlockSpec(memory_space=pl.ANY)
        dma = pltpu.SemaphoreType.DMA
        return pl.pallas_call(
            kernel,
            out_shape=pltpu.VMEM((OWN, D), BF16),
            in_specs=[away] * 8,
            out_specs=whole,
            scratch_shapes=[
                pltpu.VMEM((CHUNKS, ROWS, KC), BF16),
                pltpu.VMEM((3 * BLOCKS, ROWS, NB), F32),
                pltpu.VMEM((2, KC, WIDE), BF16),
                pltpu.VMEM((2, PS, OWN, NB), BF16),
                pltpu.VMEM((D,), BF16),
                pltpu.VMEM((ROWS, HEAD), F32),
                pltpu.VMEM((ROWS, HEAD), F32),
                dma((CHUNKS,)),
                dma((3,)),
                dma((4, KPARTS)),
                dma((CHUNKS,)), dma((CHUNKS,)), dma((CHUNKS,)), dma((CHUNKS,)), dma((CHUNKS,)), dma((CHUNKS,)),
                dma((2, PS)), dma((2, OUTS)), dma((OUTS,)), dma((OUTS,)),
                pltpu.SemaphoreType.REGULAR,
                pltpu.SemaphoreType.REGULAR,
            ],
            compiler_params=pltpu.CompilerParams(collective_id=0, has_side_effects=True, vmem_limit_bytes=62_848_000),
            cost_estimate=pl.CostEstimate(flops=8 * ROWS * D * WIDE, bytes_accessed=8 * D * WIDE, transcendentals=0),
        )(x, gain, jnp.asarray(cos), jnp.asarray(sin), wq, wk, wv, wo)

    tokens, columns = P(("dp", "tp"), None), P(None, "tp")
    return jax.shard_map(
        step,
        mesh=mesh,
        in_specs=(tokens, P(None), columns, columns, columns, P("tp", None)),
        out_specs=tokens,
        check_vma=False,
    )
```

```python
import functools

import jax
import jax.numpy as jnp
import numpy as np
from jax import lax
from jax.experimental import pallas as pl
from jax.experimental.pallas import tpu as pltpu
from jax.sharding import PartitionSpec as P

HEAD = 128
THETA = 10000
LOG2E = 1.4426950408889634
HIDDEN = -1e30
MESH = pl.DeviceIdType.MESH
BF16, F32 = jnp.bfloat16, jnp.float32

D = 16384
ROWS = 512
OWN = 128
WIDE = 4096
KC = 1024
NB = 512
CHUNKS = D // KC
BLOCKS = WIDE // NB
OUTS = D // NB
KPARTS = WIDE // KC
LAG = 12
PS = 2
UNITS = 12
EARLY = 8


def _dot(a, b, ca=1, cb=0):
    return lax.dot_general(a, b, (((ca,), (cb,)), ((), ())), preferred_element_type=F32)


def _al(i, n):
    return pl.multiple_of(i * n, n)


def kernel(x_ref, gain_in, cos_in, sin_in, wq_ref, wk_ref, wv_ref, wo_ref, o_ref, xa, acc, wb, psend, gain_ref, cos_ref,
           sin_ref, x_sem, small_sem, w_sem, gp_send, gp_recv, gc_send, gc_recv, gf_send, gf_recv, ps_send, ps_recv, cs_send, cs_recv,
           ready_p, ready_c):
    t = lax.axis_index("tp")
    chip, core = t // 2, t % 2
    partner, peer = chip * 2 + 1 - core, (1 - chip) * 2 + core
    own = pl.ds(_al(t, OWN), OWN)
    theirs = pl.ds(_al(peer, OWN), OWN)

    def load_x(c):
        return pltpu.make_async_copy(x_ref.at[:, pl.ds(_al(c, KC), KC)], o_ref.at[:, pl.ds(_al(c, KC), KC)], x_sem.at[c])

    small = [pltpu.make_async_copy(a, b, small_sem.at[i]) for i, (a, b) in
             enumerate(((gain_in, gain_ref), (cos_in, cos_ref), (sin_in, sin_ref)))]
    small[0].start()
    lax.fori_loop(0, CHUNKS, lambda c, _: load_x(c).start(), None)

    def slot(i):
        return wb.at[i // 2, :, pl.ds(_al(i % 2, WIDE // 2), WIDE // 2)]

    def start_unit(c, n, u):
        for m, w_ref in enumerate((wq_ref, wk_ref, wv_ref)):
            @pl.when(n == m)
            def _():
                rows, columns = pl.ds(_al(c, KC), KC), pl.ds(_al(u % 2, WIDE // 2), WIDE // 2)
                pltpu.make_async_copy(w_ref.at[rows, columns], slot(u % 4), w_sem.at[u % 4, 0]).start()

    def start_proj(w_ref, c, pair):
        for i in range(2):
            rows, columns = pl.ds(_al(c, KC), KC), pl.ds(i * (WIDE // 2), WIDE // 2)
            pltpu.make_async_copy(w_ref.at[rows, columns], slot(pair * 2 + i), w_sem.at[pair * 2 + i, 0]).start()

    def wait_unit(i):
        pltpu.make_async_copy(wq_ref.at[pl.ds(0, KC), pl.ds(0, WIDE // 2)], slot(i), w_sem.at[i, 0]).wait()

    def out_part(j, i):
        at = (j + 2) % 4
        return at // 2, slice(None), pl.ds(_al(at % 2 * KPARTS + i, NB), NB)

    def out_tile(j, i):
        return pltpu.make_async_copy(wo_ref.at[pl.ds(i * KC, KC), pl.ds(_al(j % OUTS, NB), NB)], wb.at[out_part(j, i)], w_sem.at[(j + 2) % 4, i])

    def start_out(j):
        for i in range(KPARTS):
            out_tile(j, i).start()

    def send(src, dst, send_sem, recv_sem, to):
        return pltpu.make_async_remote_copy(src_ref=src, dst_ref=dst, send_sem=send_sem, recv_sem=recv_sem, device_id={"tp": to},
                                            device_id_type=MESH)

    def to_partner(c):
        return send(xa.at[c, own, :], xa.at[c, own, :], gp_send.at[c], gp_recv.at[c], partner)

    def to_peer(c):
        return send(xa.at[c, own, :], xa.at[c, own, :], gc_send.at[c], gc_recv.at[c], peer)

    def forward(c):
        return send(xa.at[c, theirs, :], xa.at[c, theirs, :], gf_send.at[c], gf_recv.at[c], partner)

    barrier = pltpu.get_barrier_semaphore()
    for to in (partner, peer):
        pl.semaphore_signal(barrier, inc=1, device_id={"tp": to}, device_id_type=MESH)

    for u in range(3):
        start_unit(0, u // 2, u)

    def squares(c, total):
        load_x(c).wait()
        v = o_ref[:, pl.ds(_al(c, KC), KC)].astype(F32)
        v = v * v
        for i in range(0, KC, 128):
            total = total + v[:, i : i + 128]
        return total

    total = lax.fori_loop(0, CHUNKS, squares, jnp.zeros((OWN, 128), F32))
    scale_ref = acc.at[3 * BLOCKS - 1, pl.ds(0, OWN), pl.ds(0, 128)]
    scale_ref[...] = jnp.broadcast_to(lax.rsqrt(jnp.sum(total, axis=1, keepdims=True) * (1 / D) + 1e-6), (OWN, 128))
    pl.semaphore_wait(barrier, 2)

    def norm(c):
        v = o_ref[:, pl.ds(_al(c, KC), KC)].astype(F32)
        scale = jnp.concatenate([scale_ref[...]] * (KC // 128), axis=1)
        xa[c, own, :] = (v * scale * gain_ref[pl.ds(_al(c, KC), KC)].astype(F32).reshape(1, KC)).astype(BF16)

    def share(c):
        to_peer(c).start()
        to_partner(c).start()

    small[0].wait()
    norm(0)
    norm(1)
    share(0)
    small[1].start()
    small[2].start()

    lax.fori_loop(2, CHUNKS, lambda c, _: norm(c), None)

    def pass_on(c):
        to_peer(c).wait_recv()
        forward(c).start()


    def project_first(u, _):
        @pl.when(u + 3 < UNITS + 2)
        def _():
            start_unit((u + 3) // UNITS, (u + 3) // 2 % 3, u + 3)

        @pl.when((u % 3 == 0) & (u > 0))
        def _():
            share(u // 3)

        @pl.when(u == UNITS - 1)
        def _():
            share(4)

        @pl.when(u == 0)
        def _():
            to_partner(0).wait_recv()

        @pl.when(u == 5)
        def _():
            pass_on(0)

        @pl.when(u == 6)
        def _():
            forward(0).wait_recv()

        @pl.when(u == 9)
        def _():
            pass_on(1)

        wait_unit(u % 4)
        rows = pl.ds(_al(jnp.where(u < 6, chip, 1 - chip), 2 * OWN), 2 * OWN)
        for i in range(KPARTS):
            acc[(u % 6) * KPARTS + i, rows, :] = _dot(xa[0, rows, :], wb[u % 4 // 2, :, pl.ds(_al(u % 2 * KPARTS + i, NB), NB)])

    lax.fori_loop(0, UNITS, project_first, None)

    def project(c, _):
        for n in range(3):
            pair = (c + 1 + n) % 2
            if n == 0:
                start_proj(wk_ref, c, 1 - pair)
                to_partner(c).wait_recv()
                forward(c).wait_recv()
            elif n == 1:
                start_proj(wv_ref, c, 1 - pair)

                @pl.when(c + 1 < CHUNKS)
                def _():
                    pass_on(c + 1)
            else:
                @pl.when(c + 1 < CHUNKS)
                def _():
                    start_proj(wq_ref, c + 1, 1 - pair)

                @pl.when(c + 1 == CHUNKS)
                def _():
                    start_out(0)
                    start_out(1)

                @pl.when(c + 4 < CHUNKS)
                def _():
                    share(c + 4)

            for i in range(2):
                wait_unit(pair * 2 + i)
            for i in range(BLOCKS):
                acc[n * BLOCKS + i] += _dot(xa[c], wb[pair, :, i * NB : (i + 1) * NB])

    lax.fori_loop(1, CHUNKS, project, None)
    start_out(2)
    start_out(3)

    def sent(c, _):
        to_partner(c).wait_send()
        to_peer(c).wait_send()
        forward(c).wait_send()

    lax.fori_loop(0, CHUNKS, sent, None)
    pl.semaphore_signal(ready_p, inc=1, device_id={"tp": partner}, device_id_type=MESH)
    pl.semaphore_signal(ready_c, inc=1, device_id={"tp": peer}, device_id_type=MESH)

    def turned(v):
        v = v.astype(BF16).astype(F32)
        return lambda cos, sin: (v * cos + pltpu.roll(v, HEAD // 2, 1) * sin).astype(BF16)

    half = ROWS // 2
    seen_mask = lax.broadcasted_iota(jnp.int32, (half, half), 0) >= lax.broadcasted_iota(jnp.int32, (half, half), 1)
    e = HEAD**-0.5 * LOG2E

    def attend(qb):
        keys, first = (qb + 1) * half, qb * half

        def heads(b, _):
            def scores(u):
                lanes = slice(u * HEAD, (u + 1) * HEAD)
                q = turned(acc[b, first:keys, lanes])(cos_ref[first:keys, :], sin_ref[first:keys, :])
                k = turned(acc[BLOCKS + b, :keys, lanes])(cos_ref[:keys, :], sin_ref[:keys, :])
                return _dot(q, k, 1, 1)

            def weights(s):
                cut = jnp.where(seen_mask, s[:, first:], HIDDEN)
                s = cut if qb == 0 else jnp.concatenate([s[:, :first], cut], axis=1)
                return jnp.exp2((s - jnp.max(s, axis=1, keepdims=True)) * e).astype(BF16)

            def result(u, p):
                lanes = slice(u * HEAD, (u + 1) * HEAD)
                v = jnp.concatenate([acc[2 * BLOCKS + b, :keys, lanes].astype(BF16), jnp.ones((keys, HEAD), BF16)], axis=1)
                o = _dot(p, v)
                o = (o[:, :HEAD] * (1 / o[:, HEAD:])).astype(BF16)
                for k_core in range(2):
                    place = jnp.where(chip == qb, 2, 0) + jnp.where(core == k_core, 1, 0)
                    xa[b // 2, pl.ds(_al(place, OWN), OWN), pl.ds(_al((b % 2) * 4 + u, HEAD), HEAD)] = o[k_core * OWN : (k_core + 1) * OWN]

            every = [scores(u) for u in range(NB // HEAD)]
            every = [weights(s) for s in every]
            for u, p in enumerate(every):
                result(u, p)

        lax.fori_loop(0, BLOCKS, heads, None, unroll=2)

    def attend_for(whose):
        for qb in range(2):
            @pl.when(whose == qb)
            def _():
                attend(qb)

    small[1].wait()
    small[2].wait()
    attend_for(1 - chip)

    def piece(part, j):
        return xa.at[part + j // 8, pl.ds(_al(j % 4, OWN), OWN), pl.ds(_al((j // 4) % 2, NB), NB)]

    def terms(h, j):
        return send(psend.at[h, j % PS], piece(4 + 4 * h, j), ps_send.at[h, j % PS], ps_recv.at[h, j], partner)

    def sums(j):
        return send(piece(4, j), piece(12, j), cs_send.at[j], cs_recv.at[j], peer)

    def mine(h, j):
        return acc.at[j // 2, pl.ds(_al((chip + 1 + h) % 2 * 2 + j % 2, OWN), OWN), :]

    def keep(h, j, y):
        psend[h, j % PS] = y[:OWN].astype(BF16)
        mine(h, j)[...] = y[OWN:]

    def combine(j):
        terms(0, j).wait_recv()
        got = piece(4, j)
        got[...] = (mine(0, j)[...] + got[...].astype(F32)).astype(BF16)
        sums(j).start()

    def finish(j):
        terms(1, j).wait_recv()
        sums(j).wait_recv()
        columns = pl.ds(_al(j, NB), NB)
        total = mine(1, j)[...] + piece(8, j)[...].astype(F32) + piece(12, j)[...].astype(F32)
        o_ref[:, columns] = (o_ref[:, columns].astype(F32) + total).astype(BF16)

    def product(q, rows):
        y = _dot(xa[0, rows, :], wb[out_part(q, 0)])
        for i in range(1, KPARTS):
            y = y + _dot(xa[i, rows, :], wb[out_part(q, i)])
        return y

    def tiles(q):
        @pl.when((q >= 1) & (q + 3 < OUTS + EARLY))
        def _():
            start_out(q + 3)

        for i in range(KPARTS):
            out_tile(q, i).wait()

    pl.semaphore_wait(ready_p, 1)
    pl.semaphore_wait(ready_c, 1)

    def other_rows(j, _):
        tiles(j)

        @pl.when(j >= PS)
        def _():
            terms(0, j - PS).wait_send()

        keep(0, j, product(j, slice(0, half)))
        terms(0, j).start()

        @pl.when(j >= 1)
        def _():
            combine(j - 1)

    def all_rows(j, _):
        tiles(j)
        terms(0, j - PS).wait_send()

        @pl.when(j - PS >= EARLY)
        def _():
            terms(1, j - PS).wait_send()

        y = product(j, slice(0, ROWS))
        keep(0, j, y[:half])
        keep(1, j, y[half:])
        terms(0, j).start()
        terms(1, j).start()
        combine(j - 1)

        @pl.when(j - 1 - LAG >= EARLY)
        def _():
            finish(j - 1 - LAG)

    def own_rows(j, _):
        tiles(j + OUTS)

        @pl.when(j < PS)
        def _():
            terms(1, j + OUTS - PS).wait_send()

        @pl.when(j >= PS)
        def _():
            terms(1, j - PS).wait_send()

        keep(1, j, product(j + OUTS, slice(half, ROWS)))
        terms(1, j).start()
        finish(j + OUTS - 1 - LAG)

    lax.fori_loop(0, EARLY, other_rows, None)
    attend_for(chip)
    lax.fori_loop(EARLY, OUTS, all_rows, None)
    combine(OUTS - 1)
    lax.fori_loop(0, EARLY, own_rows, None)
    lax.fori_loop(0, EARLY, lambda j, _: finish(j), None)
    lax.fori_loop(OUTS + EARLY - 1 - LAG, OUTS, lambda j, _: finish(j), None)
    lax.fori_loop(OUTS - PS, OUTS, lambda j, _: terms(0, j).wait_send(), None)
    lax.fori_loop(EARLY - PS, EARLY, lambda j, _: terms(1, j).wait_send(), None)
    lax.fori_loop(0, OUTS, lambda j, _: sums(j).wait_send(), None)


def tables():
    half = HEAD // 2
    angle = np.arange(ROWS, dtype=np.float32)[:, None] * (THETA ** (-np.arange(half, dtype=np.float32) / half)).astype(np.float32)
    cos, sin = np.cos(angle.astype(np.float64)), np.sin(angle.astype(np.float64))
    return np.concatenate([cos, cos], 1).astype(np.float32), np.concatenate([-sin, sin], 1).astype(np.float32)


def solution(mesh):
    def step(x, gain, wq, wk, wv, wo):
        cos, sin = tables()
        whole = pl.BlockSpec(memory_space=pltpu.VMEM)
        away = pl.BlockSpec(memory_space=pl.ANY)
        dma = pltpu.SemaphoreType.DMA
        return pl.pallas_call(
            kernel,
            out_shape=pltpu.VMEM((OWN, D), BF16),
            in_specs=[away] * 8,
            out_specs=whole,
            scratch_shapes=[
                pltpu.VMEM((CHUNKS, ROWS, KC), BF16),
                pltpu.VMEM((3 * BLOCKS, ROWS, NB), F32),
                pltpu.VMEM((2, KC, WIDE), BF16),
                pltpu.VMEM((2, PS, OWN, NB), BF16),
                pltpu.VMEM((D,), BF16),
                pltpu.VMEM((ROWS, HEAD), F32),
                pltpu.VMEM((ROWS, HEAD), F32),
                dma((CHUNKS,)),
                dma((3,)),
                dma((4, KPARTS)),
                dma((CHUNKS,)), dma((CHUNKS,)), dma((CHUNKS,)), dma((CHUNKS,)), dma((CHUNKS,)), dma((CHUNKS,)),
                dma((2, PS)), dma((2, OUTS)), dma((OUTS,)), dma((OUTS,)),
                pltpu.SemaphoreType.REGULAR,
                pltpu.SemaphoreType.REGULAR,
            ],
            compiler_params=pltpu.CompilerParams(collective_id=0, has_side_effects=True, vmem_limit_bytes=62_848_000),
            cost_estimate=pl.CostEstimate(flops=8 * ROWS * D * WIDE, bytes_accessed=8 * D * WIDE, transcendentals=0),
        )(x, gain, jnp.asarray(cos), jnp.asarray(sin), wq, wk, wv, wo)

    tokens, columns = P(("dp", "tp"), None), P(None, "tp")
    return jax.shard_map(
        step,
        mesh=mesh,
        in_specs=(tokens, P(None), columns, columns, columns, P("tp", None)),
        out_specs=tokens,
        check_vma=False,
    )
```
